32 devices in a mesh: data: 1 (over z), model: 32 (over y, x, core).
Axes of the slice: x: 4, y: 4, z: 1, core: 2. Of those that a mesh axis runs over, the one named last changes fastest.
The devices are a block of a 4x4x8 slice.
Arguments:
- queries: bfloat16 [32, 896], P('data')
- w_head: bfloat16 [896, 151936], P(None, 'model')
- ds_keys: bfloat16 [524288, 896], P('model')
- ds_tokens: int32 [524288], P('model')
- temperature: float32 [1], replicated
- mix_weight: float32 [1], replicated
Outputs:
- output: float32 [32, 151936], P('data', 'model')
All inputs are finite; a program needn't handle non-finite values.
Results may differ from the reference program's by a relative error of at most 0.001.
Values are sent between devices in bfloat16 or wider.
A program may use at most 768 MiB of HBM per device.

```python
import jax
import jax.numpy as jnp
from jax import lax

Q_ROWS = 32
D_MODEL = 896
VOCAB_SIZE = 151936
N_LOCAL = 16384
GROUP_SIZE = 32


def setup_inputs(seed: int = 0, part: int = 0) -> dict:
    root_key = jax.random.key(seed)
    key_query, key_head, key_store, key_token, key_temp, key_mix = jax.random.split(root_key, 6)
    key_query = jax.random.fold_in(key_query, part)
    n_total = GROUP_SIZE * N_LOCAL
    queries = jax.random.normal(key_query, (Q_ROWS, D_MODEL), jnp.float32)
    w_head = jax.random.normal(key_head, (D_MODEL, VOCAB_SIZE), jnp.float32) * (2.0 * D_MODEL ** -0.5)
    ds_keys = jax.random.normal(key_store, (n_total, D_MODEL), jnp.float32)
    ds_tokens = jax.random.randint(key_token, (n_total,), 0, VOCAB_SIZE, jnp.int32)
    ds_tokens = ds_tokens.at[0].set(VOCAB_SIZE - 1).at[1].set(0)
    temperature = jax.random.uniform(key_temp, (1,), jnp.float32, 0.7, 0.95) * (D_MODEL ** 0.5)
    mix_weight = jax.random.uniform(key_mix, (1,), jnp.float32, 0.25, 0.5)
    return {
        "queries": queries.astype(jnp.bfloat16),
        "w_head": w_head.astype(jnp.bfloat16),
        "ds_keys": ds_keys.astype(jnp.bfloat16),
        "ds_tokens": ds_tokens,
        "temperature": temperature,
        "mix_weight": mix_weight,
    }


def reference(queries, w_head, ds_keys, ds_tokens, temperature, mix_weight):
    key_blocks = ds_keys.reshape(GROUP_SIZE, N_LOCAL, D_MODEL)
    tok_blocks = ds_tokens.reshape(GROUP_SIZE, N_LOCAL)
    temp_value = temperature[0]

    def block_scores(key_block):
        cross_dot = jnp.dot(queries, key_block.T, preferred_element_type=jnp.float32)
        key_sq = jnp.sum(jnp.square(key_block.astype(jnp.float32)), axis=1)
        return (2.0 * cross_dot - key_sq[None, :]) / temp_value

    block_max = lax.map(lambda key_block: jnp.max(block_scores(key_block), axis=1), key_blocks)
    row_max = jnp.max(block_max, axis=0)

    def accumulate(carry_state, block_pair):
        histogram, row_total = carry_state
        key_block, tok_block = block_pair
        weights = jnp.exp(block_scores(key_block) - row_max[:, None])
        histogram = histogram.at[:, tok_block].add(weights)
        return (histogram, row_total + jnp.sum(weights, axis=1)), None

    start_state = (jnp.zeros((Q_ROWS, VOCAB_SIZE), jnp.float32), jnp.zeros((Q_ROWS,), jnp.float32))
    (histogram, row_total), unused = lax.scan(accumulate, start_state, (key_blocks, tok_blocks))
    logits = jnp.dot(queries, w_head, preferred_element_type=jnp.float32)
    lm_exp = jnp.exp(logits - jnp.max(logits, axis=1, keepdims=True))
    p_lm = lm_exp / jnp.sum(lm_exp, axis=1, keepdims=True)
    mix_value = mix_weight[0]
    return jnp.log(mix_value * histogram / row_total[:, None] + (1.0 - mix_value) * p_lm)
```

```python
import functools

import jax
import jax.numpy as jnp
from jax import lax
from jax.experimental import pallas as pl
from jax.experimental.pallas import tpu as pltpu
from jax.sharding import PartitionSpec as P

MESH = pl.DeviceIdType.MESH
LANES = 128
BLK = 1024
SUB = 256
F32 = jnp.float32


def _bit_reverse(k, bits):
    out = 0
    for i in range(bits):
        out |= ((k >> i) & 1) << (bits - 1 - i)
    return out


def _exchange_kernel(
    cfg, start_ref, inv_ref, tau_ref, q4_ref, q_ref, tok_ref, keys_hbm, w_hbm,
    recv_ref, stats_out, logits_ref,
    kbuf, scores, wbuf, send, stats, stats_recv,
    ksem, wsem, lsem, send_sem, recv_sem, ssend_sem, srecv_sem, osem,
):
    group, rows, cap, cols, copies, vrows = cfg
    me = lax.axis_index("model")
    n_local = keys_hbm.shape[0]
    nblk = n_local // BLK
    crows = cap // copies
    qrows = q_ref.shape[0]

    barrier = pltpu.get_barrier_semaphore()

    @pl.loop(1, group)
    def _(k):
        peer = lax.rem(me + k, group)
        pl.semaphore_signal(barrier, inc=1, device_id={"model": peer}, device_id_type=MESH)

    def key_copy(b, slot):
        return pltpu.make_async_copy(keys_hbm.at[pl.ds(b * BLK, BLK), :], kbuf.at[slot], ksem.at[slot])

    key_copy(0, 0).start()
    key_copy(1, 1).start()
    w_copy = pltpu.make_async_copy(w_hbm, wbuf, wsem)
    tau = tau_ref[0]

    def block(b, best):
        slot = lax.rem(b, 3)

        @pl.when(b + 2 < nblk)
        def _():
            key_copy(b + 2, lax.rem(b + 2, 3)).start()

        key_copy(b, slot).wait()

        def piece(p, best):
            x = kbuf[slot, pl.ds(p * SUB, SUB), :]
            dot = jnp.dot(x, q4_ref[...], preferred_element_type=F32)
            xf = x.astype(F32)
            sq = jnp.square(xf[:, :LANES])
            for j in range(1, x.shape[1] // LANES):
                sq = sq + jnp.square(xf[:, j * LANES:(j + 1) * LANES])
            norm = jnp.sum(sq, axis=1, keepdims=True)
            s = (2.0 * dot - norm) / tau
            scores[pl.ds(b * BLK + p * SUB, SUB), :] = s
            return jnp.maximum(best, jnp.max(s.reshape(SUB // 8, 8, LANES), axis=0))

        return lax.fori_loop(0, BLK // SUB, piece, best)

    best = lax.fori_loop(0, nblk, block, jnp.full((8, LANES), -jnp.inf, F32))
    w_copy.start()
    row_max = jnp.max(best, axis=0, keepdims=True)

    pl.semaphore_wait(barrier, group - 1)

    lane_group = lax.broadcasted_iota(jnp.int32, (1, LANES), 1) // qrows
    entry = (
        lax.broadcasted_iota(jnp.int32, (crows, LANES), 0) * copies
        + lax.broadcasted_iota(jnp.int32, (crows, LANES), 1) // qrows
    )
    id_pos = lax.broadcasted_iota(jnp.int32, (8, LANES), 0) * LANES + lax.broadcasted_iota(jnp.int32, (8, LANES), 1)
    id_lane = lax.broadcasted_iota(jnp.int32, (8, LANES), 1)

    def block_send(k, dest):
        return pltpu.make_async_remote_copy(
            src_ref=send.at[k], dst_ref=recv_ref.at[me], send_sem=send_sem.at[k], recv_sem=recv_sem.at[me],
            device_id={"model": dest}, device_id_type=MESH,
        )

    bits = group.bit_length() - 1

    def offset_of(j):
        k = 0
        for i in range(bits):
            k = k + lax.rem(lax.div(j, 1 << i), 2) * (1 << (bits - 1 - i))
        return k

    def pack(k, total):
        dest = lax.rem(me + k, group)
        first = start_ref[dest]
        count = start_ref[dest + 1] - first

        @pl.loop(0, crows // 8)
        def _(t):
            base = first + t * (8 * copies)
            for r in range(8):
                parts = [scores[pl.ds(inv_ref[base + r * copies + g], 1), :] for g in range(copies)]
                row = parts[copies - 1]
                for g in range(copies - 2, -1, -1):
                    row = jnp.where(lane_group == g, parts[g], row)
                send[k, pl.ds(t * 8 + r, 1), :] = row

        w = jnp.where(entry < count, jnp.exp(send[k, :crows, :] - row_max), 0.0)
        send[k, :crows, :] = w
        shift = lax.rem(first, LANES)
        at = lax.div(first, LANES)
        low = pltpu.roll(tok_ref[pl.ds(at, 8), :], LANES - shift, axis=1)
        high = pltpu.roll(tok_ref[pl.ds(at + 1, 8), :], LANES - shift, axis=1)
        tok = jnp.where(id_lane < LANES - shift, low, high) - dest * cols
        send[k, crows:crows + 8, :] = jnp.where(id_pos < count, tok, cols).astype(F32)
        return total + jnp.sum(w.reshape(crows // 8, 8, LANES), axis=0)

    def step(j, total):
        k = offset_of(j)
        total = pack(k, total)
        block_send(k, lax.rem(me + k, group)).start()
        return total

    total = lax.fori_loop(1, group, step, jnp.zeros((8, LANES), F32))
    total = pack(0, total)
    own = pltpu.make_async_copy(send.at[0], recv_ref.at[me], lsem)
    own.start()

    w_copy.wait()
    def head(at, size, carry):
        lm_max, lm_sum = carry
        x = jnp.dot(wbuf[pl.ds(at, size), :], q4_ref[...], preferred_element_type=F32)
        logits_ref[pl.ds(at, size), :] = x
        new = jnp.maximum(lm_max, jnp.max(x, axis=0, keepdims=True))
        return new, lm_sum * jnp.exp(lm_max - new) + jnp.sum(jnp.exp(x - new), axis=0, keepdims=True)

    carry = (jnp.full((1, LANES), -jnp.inf, F32), jnp.zeros((1, LANES), F32))
    carry = lax.fori_loop(0, cols // SUB, lambda i, c: head(i * SUB, SUB, c), carry)
    if cols % SUB:
        carry = head(cols // SUB * SUB, cols % SUB, carry)
    lm_max_row, lm_sum_row = carry

    def worst(d, c):
        return jnp.maximum(c, start_ref[d + 1] - start_ref[d])

    most = lax.fori_loop(0, group, worst, jnp.int32(0))
    over = jnp.where(most > cap, 1.0, 0.0).astype(F32)
    stats[0:1, :] = row_max
    stats[1:2, :] = jnp.sum(total, axis=0, keepdims=True)
    stats[2:3, :] = lm_max_row
    stats[3:4, :] = lm_sum_row
    stats[4:5, :] = jnp.full((1, LANES), over, F32)
    stats[5:8, :] = jnp.zeros((3, LANES), F32)

    def stat_send(k, dest):
        return pltpu.make_async_remote_copy(
            src_ref=stats, dst_ref=stats_recv.at[me], send_sem=ssend_sem.at[k], recv_sem=srecv_sem.at[me],
            device_id={"model": dest}, device_id_type=MESH,
        )

    @pl.loop(1, group)
    def _(k):
        stat_send(k, lax.rem(me + k, group)).start()

    stats_recv[me] = stats[...]

    @pl.loop(1, group)
    def _(k):
        src = lax.rem(me + group - k, group)
        pltpu.make_async_remote_copy(
            src_ref=stats, dst_ref=stats_recv.at[src], send_sem=ssend_sem.at[k], recv_sem=srecv_sem.at[src],
            device_id={"model": src}, device_id_type=MESH,
        ).wait_recv()
        pltpu.make_async_remote_copy(
            src_ref=send.at[k], dst_ref=recv_ref.at[src], send_sem=send_sem.at[k], recv_sem=recv_sem.at[src],
            device_id={"model": src}, device_id_type=MESH,
        ).wait_recv()

    @pl.loop(1, group)
    def _(k):
        block_send(k, lax.rem(me + k, group)).wait_send()
        stat_send(k, lax.rem(me + k, group)).wait_send()

    own.wait()
    stats_out[...] = stats_recv[...]


def _finish_kernel(
    cfg, mix_ref, stats_ref, recv_ref, logits_ref, out_ref, hist0, hist1, hist2, hist3, scaled, idbuf, ids, sem
):
    group, rows, cap, cols, copies, vrows = cfg
    crows = cap // copies
    hists = (hist0, hist1, hist2, hist3)
    idbuf[...] = recv_ref[:, crows:crows + 8, :].astype(jnp.int32)
    id_copy = pltpu.make_async_copy(idbuf, ids, sem)
    id_copy.start()

    st = stats_ref[...]
    m_all = st[:, 0, :]
    m = jnp.max(m_all, axis=0, keepdims=True)
    scale = jnp.exp(m_all - m)
    z = jnp.sum(st[:, 1, :] * scale, axis=0, keepdims=True)
    lm_all = st[:, 2, :]
    lm = jnp.max(lm_all, axis=0, keepdims=True)
    lmz = jnp.sum(st[:, 3, :] * jnp.exp(lm_all - lm), axis=0, keepdims=True)

    @pl.loop(0, vrows // 8)
    def _(i):
        for h in hists:
            h[pl.ds(i * 8, 8), :] = jnp.zeros((8, LANES), F32)

    for s in range(group):
        scaled[s] = recv_ref[s, :crows, :] * scale[s:s + 1, :]
    id_copy.wait()

    @pl.loop(0, group)
    def _(s):
        @pl.loop(0, crows // 8)
        def _(t):
            sub = lax.div(t, LANES // (8 * copies))
            lane0 = lax.rem(t, LANES // (8 * copies)) * (8 * copies)
            for r in range(8):
                row = scaled[s, pl.ds(t * 8 + r, 1), :]
                for g in range(copies):
                    v = ids[s, sub, lane0 + r * copies + g]
                    hists[g][pl.ds(v, 1), :] = hists[g][pl.ds(v, 1), :] + row

    qrows = out_ref.shape[0]
    lane = lax.broadcasted_iota(jnp.int32, (LANES, LANES), 1)
    eye = lane == lax.broadcasted_iota(jnp.int32, (LANES, LANES), 0)

    def column(row):
        return jnp.sum(jnp.where(eye, row, 0.0), axis=1, keepdims=True)

    zc = column(z)
    z_col = zc[:qrows]
    for g in range(1, copies):
        z_col = z_col + zc[g * qrows:(g + 1) * qrows]
    lmz_col = column(lmz)[:qrows]
    mix = mix_ref[0]
    a = mix / z_col
    b = (1.0 - mix) / lmz_col
    for c in range(pl.cdiv(cols, LANES)):
        width = min(LANES, cols - c * LANES)
        hrows = min(LANES, vrows - c * LANES)
        acc = hists[0][c * LANES:c * LANES + hrows, :]
        for g in range(1, copies):
            acc = jnp.where(lane[:hrows] // qrows >= g, hists[g][c * LANES:c * LANES + hrows, :], acc)
        if hrows < LANES:
            acc = jnp.concatenate([acc, jnp.zeros((LANES - hrows, LANES), F32)], axis=0)
        tr = acc.T
        h = tr[:qrows]
        for g in range(1, copies):
            h = h + tr[g * qrows:(g + 1) * qrows]
        e = jnp.exp(logits_ref[c * LANES:c * LANES + width, :] - lm)
        if width < LANES:
            e = jnp.concatenate([e, jnp.zeros((LANES - width, LANES), F32)], axis=0)
        e = e.T[:qrows, :width]
        out_ref[:, c * LANES:c * LANES + width] = jnp.log(h[:, :width] * a + e * b)


def solution(mesh):
    group = mesh.shape["model"]

    def dense_path(queries, w_shard, key_shard, tok_shard, temperature, mix_weight):
        row_count = queries.shape[0]
        cols = w_shard.shape[1]
        cross_dot = jnp.einsum("bd,nd->bn", queries, key_shard, preferred_element_type=F32)
        key_sq = jnp.sum(jnp.square(key_shard.astype(F32)), axis=1)
        scores = (2.0 * cross_dot - key_sq[None, :]) / temperature[0]
        row_max = lax.pmax(jnp.max(scores, axis=1), "model")
        weights = jnp.exp(scores - row_max[:, None])
        row_total = lax.psum(jnp.sum(weights, axis=1), "model")
        local_hist = jnp.zeros((row_count, cols * group), F32).at[:, tok_shard].add(weights)
        pieces = jnp.transpose(local_hist.reshape(row_count, group, cols), (1, 0, 2))
        histogram = jnp.sum(lax.all_to_all(pieces, "model", 0, 0), axis=0)
        logits = jnp.dot(queries, w_shard, preferred_element_type=F32)
        lm_max = lax.pmax(jnp.max(logits, axis=1), "model")
        lm_exp = jnp.exp(logits - lm_max[:, None])
        lm_total = lax.psum(jnp.sum(lm_exp, axis=1), "model")
        mix = mix_weight[0]
        return jnp.log(mix * (histogram / row_total[:, None]) + (1.0 - mix) * (lm_exp / lm_total[:, None]))

    def local_step(queries, w_shard, key_shard, tok_shard, temperature, mix_weight):
        rows, dim = queries.shape
        n_local = key_shard.shape[0]
        cols = w_shard.shape[1]
        copies = LANES // rows
        mean = n_local // group
        cap = -(-int(mean + 5.6 * mean ** 0.5) // 32) * 32
        crows = cap // copies
        vrows = (cols // 8 + 1) * 8
        cfg = (group, rows, cap, cols, copies, vrows)

        tok_sorted, inv = lax.sort((tok_shard, lax.iota(jnp.int32, n_local)), num_keys=1)
        bounds = lax.iota(jnp.int32, group + 1) * cols
        start = jnp.sum((tok_sorted[None, :] < bounds[:, None]).astype(jnp.int32), axis=1)
        inv = jnp.pad(inv, (0, cap))
        tok2d = jnp.pad(tok_sorted, (0, 16 * LANES)).reshape(n_local // LANES + 16, LANES)
        q4 = jnp.tile(queries.T, (1, copies))

        smem = pl.BlockSpec(memory_space=pltpu.SMEM)
        vmem = pl.BlockSpec(memory_space=pltpu.VMEM)
        hbm = pl.BlockSpec(memory_space=pl.ANY)
        recv, stats, logits = pl.pallas_call(
            functools.partial(_exchange_kernel, cfg),
            out_shape=(
                jax.ShapeDtypeStruct((group, crows + 8, LANES), F32),
                jax.ShapeDtypeStruct((group, 8, LANES), F32),
                jax.ShapeDtypeStruct((cols, LANES), F32),
            ),
            in_specs=[smem, smem, smem, vmem, vmem, vmem, hbm, hbm],
            out_specs=(hbm, vmem, vmem),
            scratch_shapes=[
                pltpu.VMEM((3, BLK, dim), jnp.bfloat16),
                pltpu.VMEM((n_local, LANES), F32),
                pltpu.VMEM((cols, dim), jnp.bfloat16),
                pltpu.VMEM((group, crows + 8, LANES), F32),
                pltpu.VMEM((8, LANES), F32),
                pltpu.VMEM((group, 8, LANES), F32),
                pltpu.SemaphoreType.DMA((3,)),
                pltpu.SemaphoreType.DMA,
                pltpu.SemaphoreType.DMA,
                pltpu.SemaphoreType.DMA((group,)),
                pltpu.SemaphoreType.DMA((group,)),
                pltpu.SemaphoreType.DMA((group,)),
                pltpu.SemaphoreType.DMA((group,)),
                pltpu.SemaphoreType.DMA,
            ],
            compiler_params=pltpu.CompilerParams(
                collective_id=0, has_side_effects=True, vmem_limit_bytes=60 * 1024 * 1024
            ),
            name="knn_exchange",
        )(start, inv, temperature, q4, queries, tok2d, key_shard, w_shard.T)

        fast = pl.pallas_call(
            functools.partial(_finish_kernel, cfg),
            out_shape=jax.ShapeDtypeStruct((rows, cols), F32),
            in_specs=[smem, vmem, vmem, vmem],
            out_specs=vmem,
            scratch_shapes=[pltpu.VMEM((vrows, LANES), F32)] * 4
            + [
                pltpu.VMEM((group, crows, LANES), F32),
                pltpu.VMEM((group, 8, LANES), jnp.int32),
                pltpu.SMEM((group, 8, LANES), jnp.int32),
                pltpu.SemaphoreType.DMA,
            ],
            compiler_params=pltpu.CompilerParams(vmem_limit_bytes=60 * 1024 * 1024),
            name="knn_finish",
        )(mix_weight, stats, recv, logits)

        overflow = jnp.max(stats[:, 4, 0]) > 0.0
        args = (queries, w_shard, key_shard, tok_shard, temperature, mix_weight)
        return lax.cond(overflow, lambda: dense_path(*args), lambda: fast)

    return jax.shard_map(
        local_step,
        mesh=mesh,
        in_specs=(P("data", None), P(None, "model"), P("model", None), P("model"), P(), P()),
        out_specs=P("data", "model"),
        check_vma=False,
    )
```

```python
import functools

import jax
import jax.numpy as jnp
from jax import lax
from jax.experimental import pallas as pl
from jax.experimental.pallas import tpu as pltpu
from jax.sharding import PartitionSpec as P

MESH = pl.DeviceIdType.MESH
LANES = 128
BLK = 1024
SUB = 512
F32 = jnp.float32


DUP = 1 << 16
TILE_ROWS = 16


def _exchange_kernel(
    cfg, tau_ref, q_ref, sorted_ref, inv_hbm, keys_hbm, w_hbm,
    recv_ref, stats_out, logits_ref,
    q4_ref, tok_ref, inv_ref, isem, start_vmem, start_ref, stsem, kbuf, scores, wbuf, send, stats, stats_recv,
    ksem, wsem, lsem, send_sem, recv_sem, ssend_sem, srecv_sem, osem,
):
    group, rows, cap, cols, copies, vrows, side = cfg
    me = lax.axis_index("model")
    n_local = keys_hbm.shape[0]
    nblk = n_local // BLK
    crows = cap // copies
    tile = TILE_ROWS * copies
    qrows = q_ref.shape[0]

    barrier = pltpu.get_barrier_semaphore()

    @pl.loop(1, group)
    def _(k):
        peer = lax.rem(me + k, group)
        pl.semaphore_signal(barrier, inc=1, device_id={"model": peer}, device_id_type=MESH)

    def key_copy(b, slot):
        return pltpu.make_async_copy(keys_hbm.at[pl.ds(b * BLK, BLK), :], kbuf.at[slot], ksem.at[slot])

    key_copy(0, 0).start()
    key_copy(1, 1).start()
    w_copy = pltpu.make_async_copy(w_hbm, wbuf, wsem)
    inv_copy = pltpu.make_async_copy(inv_hbm, inv_ref.at[pl.ds(0, n_local)], isem)
    inv_copy.start()
    for i in range(tile):
        inv_ref[n_local + i] = 0
    tau = tau_ref[0]

    qt = jnp.concatenate([q_ref[...].astype(F32)] * copies, axis=0)
    for j in range(qt.shape[1] // LANES):
        q4_ref[j * LANES:(j + 1) * LANES, :] = qt[:, j * LANES:(j + 1) * LANES].T.astype(jnp.bfloat16)
    krows = sorted_ref.shape[0]
    tok_ref[:krows, :] = sorted_ref[...]
    tok_ref[krows:, :] = jnp.zeros((tok_ref.shape[0] - krows, LANES), jnp.int32)
    start_vmem[...] = jnp.zeros(start_vmem.shape, jnp.int32)
    for d in range(group + 1):
        below = jnp.where(sorted_ref[...] < d * cols, 1, 0).reshape(krows // 8, 8, LANES)
        part = below[0]
        for i in range(1, krows // 8):
            part = part + below[i]
        for i in (4, 2, 1):
            part = part[:i] + part[i:2 * i]
        start_vmem[d:d + 1, :] = part
    counts = start_vmem[...]
    turn = LANES // 2
    while turn:
        counts = counts + pltpu.roll(counts, turn, axis=1)
        turn //= 2
    start_vmem[...] = counts
    start_copy = pltpu.make_async_copy(start_vmem, start_ref, stsem)

    def block(b, best):
        slot = lax.rem(b, 3)

        @pl.when(b + 2 < nblk)
        def _():
            key_copy(b + 2, lax.rem(b + 2, 3)).start()

        @pl.when(b == 1)
        def _():
            start_copy.start()

        key_copy(b, slot).wait()

        def piece(p, best):
            x = kbuf[slot, pl.ds(p * SUB, SUB), :]
            dot = jnp.dot(x, q4_ref[...], preferred_element_type=F32)
            xf = x.astype(F32)
            sq = jnp.square(xf[:, :LANES])
            for j in range(1, x.shape[1] // LANES):
                sq = sq + jnp.square(xf[:, j * LANES:(j + 1) * LANES])
            norm = jnp.sum(sq, axis=1, keepdims=True)
            s = (2.0 * dot - norm) / tau
            scores[pl.ds(b * BLK + p * SUB, SUB), :] = s
            return jnp.maximum(best, jnp.max(s.reshape(SUB // 8, 8, LANES), axis=0))

        return lax.fori_loop(0, BLK // SUB, piece, best)

    best = lax.fori_loop(0, nblk, block, jnp.full((8, LANES), -jnp.inf, F32))
    w_copy.start()
    row_max = jnp.max(best, axis=0, keepdims=True)

    inv_copy.wait()
    start_copy.wait()
    pl.semaphore_wait(barrier, group - 1)

    lane_group = lax.broadcasted_iota(jnp.int32, (1, LANES), 1) // qrows
    entry = (
        lax.broadcasted_iota(jnp.int32, (crows, LANES), 0) * copies
        + lax.broadcasted_iota(jnp.int32, (crows, LANES), 1) // qrows
    )
    id_pos = lax.broadcasted_iota(jnp.int32, (8, LANES), 0) * LANES + lax.broadcasted_iota(jnp.int32, (8, LANES), 1)
    id_lane = lax.broadcasted_iota(jnp.int32, (8, LANES), 1)

    def block_send(k, dest):
        return pltpu.make_async_remote_copy(
            src_ref=send.at[k], dst_ref=recv_ref.at[me], send_sem=send_sem.at[k], recv_sem=recv_sem.at[me],
            device_id={"model": dest}, device_id_type=MESH,
        )

    def far_first(i, n):
        odd = lax.rem(i, 2)
        return n // 2 + (1 - odd) * lax.div(i, 2) - odd * lax.div(i + 1, 2)

    def dest_of(j):
        if side == 0:
            return lax.rem(me + 1 + j, group)
        y, x, c = lax.div(me, 2 * side), lax.rem(lax.div(me, 2), side), lax.rem(me, 2)
        dy = far_first(lax.rem(j, side), side)
        dx = far_first(lax.div(j, 2 * side), side)
        dc = 1 - lax.rem(lax.div(j, side), 2)
        return (lax.rem(y + dy, side) * side + lax.rem(x + dx, side)) * 2 + lax.rem(c + dc, 2)

    def pack(k, dest, total):
        first = jnp.clip(start_ref[dest, 0], 0, n_local)
        count = start_ref[dest + 1, 0] - first

        @pl.loop(0, crows // TILE_ROWS)
        def _(t):
            base = jnp.minimum(first + t * tile, n_local)
            near = [inv_ref.at[pl.ds(i, n_local + 1)][base] for i in range(tile)]
            for r in range(TILE_ROWS):
                parts = [scores[pl.ds(near[r * copies + g], 1), :] for g in range(copies)]
                row = parts[copies - 1]
                for g in range(copies - 2, -1, -1):
                    row = jnp.where(lane_group == g, parts[g], row)
                send[k, pl.ds(t * TILE_ROWS + r, 1), :] = row

        w = jnp.where(entry < count, jnp.exp(send[k, :crows, :] - row_max), 0.0)
        send[k, :crows, :] = w
        shift = lax.rem(first, LANES)
        at = lax.div(first, LANES)
        low = pltpu.roll(tok_ref[pl.ds(at, 8), :], LANES - shift, axis=1)
        high = pltpu.roll(tok_ref[pl.ds(at + 1, 8), :], LANES - shift, axis=1)
        tok = jnp.where(id_lane < LANES - shift, low, high) - dest * cols
        tok = jnp.where(id_pos < count, tok, cols + lax.rem(lax.div(id_pos, copies), TILE_ROWS))
        send[k, crows:crows + 8, :] = jnp.where(id_pos < 7 * LANES, tok, count).astype(F32)
        return total + jnp.sum(w.reshape(crows // 8, 8, LANES), axis=0)

    def step(j, total):
        total = pack(j, dest_of(j), total)
        block_send(j - 1, dest_of(j - 1)).start()
        return total

    total = pack(0, dest_of(0), jnp.zeros((8, LANES), F32))
    total = lax.fori_loop(1, group - 1, step, total)
    total = pack(group - 1, me, total)
    block_send(group - 2, dest_of(group - 2)).start()
    own = pltpu.make_async_copy(send.at[group - 1], recv_ref.at[me], lsem)

    w_copy.wait()
    def head(at, size, carry):
        lm_max, lm_sum = carry
        x = jnp.dot(wbuf[pl.ds(at, size), :], q4_ref[...], preferred_element_type=F32)
        logits_ref[pl.ds(at, size), :] = x
        new = jnp.maximum(lm_max, jnp.max(x, axis=0, keepdims=True))
        return new, lm_sum * jnp.exp(lm_max - new) + jnp.sum(jnp.exp(x - new), axis=0, keepdims=True)

    carry = (jnp.full((1, LANES), -jnp.inf, F32), jnp.zeros((1, LANES), F32))
    carry = lax.fori_loop(0, cols // SUB, lambda i, c: head(i * SUB, SUB, c), carry)
    if cols % SUB:
        carry = head(cols // SUB * SUB, cols % SUB, carry)
    lm_max_row, lm_sum_row = carry

    def worst(d, c):
        return jnp.maximum(c, start_ref[d + 1, 0] - start_ref[d, 0])

    most = lax.fori_loop(0, group, worst, jnp.int32(0))
    over = jnp.where(most > cap, 1.0, 0.0).astype(F32)
    stats[0:1, :] = row_max
    stats[1:2, :] = jnp.sum(total, axis=0, keepdims=True)
    stats[2:3, :] = lm_max_row
    stats[3:4, :] = lm_sum_row
    stats[4:5, :] = jnp.full((1, LANES), over, F32)
    stats[5:8, :] = jnp.zeros((3, LANES), F32)
    own.start()
    own.wait()

    def stat_send(k, dest):
        return pltpu.make_async_remote_copy(
            src_ref=stats, dst_ref=stats_recv.at[me], send_sem=ssend_sem.at[k], recv_sem=srecv_sem.at[me],
            device_id={"model": dest}, device_id_type=MESH,
        )

    @pl.loop(1, group)
    def _(k):
        stat_send(k, lax.rem(me + k, group)).start()

    stats_recv[me] = stats[...]

    @pl.loop(1, group)
    def _(k):
        src = lax.rem(me + group - k, group)
        pltpu.make_async_remote_copy(
            src_ref=stats, dst_ref=stats_recv.at[src], send_sem=ssend_sem.at[k], recv_sem=srecv_sem.at[src],
            device_id={"model": src}, device_id_type=MESH,
        ).wait_recv()
        pltpu.make_async_remote_copy(
            src_ref=send.at[k - 1], dst_ref=recv_ref.at[src], send_sem=send_sem.at[k - 1], recv_sem=recv_sem.at[src],
            device_id={"model": src}, device_id_type=MESH,
        ).wait_recv()

    @pl.loop(1, group)
    def _(k):
        block_send(k - 1, dest_of(k - 1)).wait_send()
        stat_send(k, lax.rem(me + k, group)).wait_send()

    stats_out[...] = stats_recv[...]


def _finish_kernel(
    cfg, mix_ref, stats_ref, recv_ref, logits_hbm, out_ref, over_ref,
    hist0, hist1, hist2, hist3, scaled, logits_ref, idbuf, ids, sem, lsem,
):
    group, rows, cap, cols, copies, vrows, side = cfg
    crows = cap // copies
    hists = (hist0, hist1, hist2, hist3)
    logits_copy = pltpu.make_async_copy(logits_hbm, logits_ref, lsem)
    logits_copy.start()
    tile = TILE_ROWS * copies
    lane3 = lax.broadcasted_iota(jnp.int32, (8, LANES), 1)
    row3 = lax.broadcasted_iota(jnp.int32, (8, LANES), 0)
    for s in range(group):
        v = recv_ref[s, crows:crows + 8, :].astype(jnp.int32)
        same = (v == pltpu.roll(v, LANES - copies, axis=1)) & (lax.rem(lane3, tile) < tile - copies)
        flag = jnp.where(same, 1, 0)
        step = tile // 2
        while step:
            flag = flag | pltpu.roll(flag, LANES - step, axis=1)
            step //= 2
        count = jnp.sum(jnp.where((lane3 == 0) & (row3 == 7), v, 0).astype(F32)).astype(jnp.int32)
        flag = jnp.where(row3 * LANES + lane3 < count, flag, 2)
        idbuf[s] = v + jnp.where((lax.rem(lane3, tile) == 0) & (row3 < 7), flag * DUP, 0)
    id_copy = pltpu.make_async_copy(idbuf, ids, sem)

    st = stats_ref[...]
    m_all = st[:, 0, :]
    m = jnp.max(m_all, axis=0, keepdims=True)
    scale = jnp.exp(m_all - m)
    z = jnp.sum(st[:, 1, :] * scale, axis=0, keepdims=True)
    lm_all = st[:, 2, :]
    lm = jnp.max(lm_all, axis=0, keepdims=True)
    lmz = jnp.sum(st[:, 3, :] * jnp.exp(lm_all - lm), axis=0, keepdims=True)

    @pl.loop(0, vrows // 32)
    def _(i):
        for h in hists:
            h[pl.ds(i * 32, 32), :] = jnp.zeros((32, LANES), F32)

    id_copy.start()
    for s in range(group):
        scaled[s] = recv_ref[s, :crows, :] * scale[s:s + 1, :]
    id_copy.wait()

    per = LANES // tile

    def tile_add(s, near, t, k):
        code = near[k * tile]
        at = lambda i: near[k * tile + i] if i else code & (DUP - 1)

        @pl.when(code < DUP)
        def _():
            rows_ = [scaled[s, pl.ds(t * TILE_ROWS + r, 1), :] for r in range(TILE_ROWS)]
            for g in range(copies):
                at_g = [at(r * copies + g) for r in range(TILE_ROWS)]
                new = [hists[g][pl.ds(v, 1), :] + row for v, row in zip(at_g, rows_)]
                for v, x in zip(at_g, new):
                    hists[g][pl.ds(v, 1), :] = x

        @pl.when((code >= DUP) & (code < 2 * DUP))
        def _():
            for r in range(TILE_ROWS):
                row = scaled[s, pl.ds(t * TILE_ROWS + r, 1), :]
                for g in range(copies):
                    v = at(r * copies + g)
                    hists[g][pl.ds(v, 1), :] = hists[g][pl.ds(v, 1), :] + row

    @pl.loop(0, group)
    def _(s):
        @pl.loop(0, lax.div(jnp.minimum(ids[s, 7, 0], cap) + (LANES - 1), LANES))
        def _(sub):
            near = [ids.at[:, :, pl.ds(i, 1)][s, sub, 0] for i in range(LANES)]
            for k in range(per):
                tile_add(s, near, sub * per + k, k)

    over_ref[0] = jnp.max(st[:, 4, :]).astype(jnp.int32)
    logits_copy.wait()

    qrows = out_ref.shape[0]
    lane = lax.broadcasted_iota(jnp.int32, (LANES, LANES), 1)
    z8 = jnp.broadcast_to(z, (8, LANES))
    z_all = z8
    for g in range(1, copies):
        z_all = z_all + pltpu.roll(z8, g * qrows, axis=1)
    mix = mix_ref[0]
    a = mix / z_all[0:1]
    b = jnp.where(lane[0:1] < qrows, (1.0 - mix) / lmz, 0.0)
    for c in range(pl.cdiv(cols, LANES)):
        width = min(LANES, cols - c * LANES)
        part = slice(c * LANES, c * LANES + width)
        acc = hists[0][part, :]
        for g in range(1, copies):
            acc = jnp.where(lane[:width] >= g * qrows, hists[g][part, :], acc)
        x = acc * a + jnp.exp(logits_ref[part, :] - lm) * b
        if width < LANES:
            x = jnp.concatenate([x, jnp.zeros((LANES - width, LANES), F32)], axis=0)
        tr = x.T
        p = tr[:qrows]
        for g in range(1, copies):
            p = p + tr[g * qrows:(g + 1) * qrows]
        out_ref[:, part] = jnp.log(p[:, :width])


def solution(mesh):
    group = mesh.shape["model"]

    def dense_path(queries, w_shard, key_shard, tok_shard, temperature, mix_weight):
        row_count = queries.shape[0]
        cols = w_shard.shape[1]
        cross_dot = jnp.einsum("bd,nd->bn", queries, key_shard, preferred_element_type=F32)
        key_sq = jnp.sum(jnp.square(key_shard.astype(F32)), axis=1)
        scores = (2.0 * cross_dot - key_sq[None, :]) / temperature[0]
        row_max = lax.pmax(jnp.max(scores, axis=1), "model")
        weights = jnp.exp(scores - row_max[:, None])
        row_total = lax.psum(jnp.sum(weights, axis=1), "model")
        local_hist = jnp.zeros((row_count, cols * group), F32).at[:, tok_shard].add(weights)
        pieces = jnp.transpose(local_hist.reshape(row_count, group, cols), (1, 0, 2))
        histogram = jnp.sum(lax.all_to_all(pieces, "model", 0, 0), axis=0)
        logits = jnp.dot(queries, w_shard, preferred_element_type=F32)
        lm_max = lax.pmax(jnp.max(logits, axis=1), "model")
        lm_exp = jnp.exp(logits - lm_max[:, None])
        lm_total = lax.psum(jnp.sum(lm_exp, axis=1), "model")
        mix = mix_weight[0]
        return jnp.log(mix * (histogram / row_total[:, None]) + (1.0 - mix) * (lm_exp / lm_total[:, None]))

    def local_step(queries, w_shard, key_shard, tok_shard, temperature, mix_weight):
        rows, dim = queries.shape
        n_local = key_shard.shape[0]
        cols = w_shard.shape[1]
        copies = LANES // rows
        mean = n_local // group
        cap = -(-int(mean + 5.6 * mean ** 0.5) // (TILE_ROWS * copies)) * (TILE_ROWS * copies)
        crows = cap // copies
        vrows = -(-(cols + TILE_ROWS) // 32) * 32
        side = int((group // 2) ** 0.5)
        side = side if side * side * 2 == group and side in (2, 4) else 0
        cfg = (group, rows, cap, cols, copies, vrows, side)
        srows = -(-(group + 1) // 8) * 8
        assert n_local % (8 * LANES) == 0 and cap <= 7 * LANES and vrows < DUP
        tok_sorted, inv = lax.sort((tok_shard, lax.iota(jnp.int32, n_local)), num_keys=1)

        smem = pl.BlockSpec(memory_space=pltpu.SMEM)
        vmem = pl.BlockSpec(memory_space=pltpu.VMEM)
        hbm = pl.BlockSpec(memory_space=pl.ANY)
        recv, stats, logits = pl.pallas_call(
            functools.partial(_exchange_kernel, cfg),
            out_shape=(
                jax.ShapeDtypeStruct((group, crows + 8, LANES), F32),
                jax.ShapeDtypeStruct((group, 8, LANES), F32),
                jax.ShapeDtypeStruct((cols, LANES), F32),
            ),
            in_specs=[smem, vmem, vmem, hbm, hbm, hbm],
            out_specs=(hbm, vmem, vmem),
            scratch_shapes=[
                pltpu.VMEM((dim, LANES), jnp.bfloat16),
                pltpu.VMEM((n_local // LANES + 16, LANES), jnp.int32),
                pltpu.SMEM((n_local + TILE_ROWS * copies,), jnp.int32),
                pltpu.SemaphoreType.DMA,
                pltpu.VMEM((srows, LANES), jnp.int32),
                pltpu.SMEM((srows, LANES), jnp.int32),
                pltpu.SemaphoreType.DMA,
                pltpu.VMEM((3, BLK, dim), jnp.bfloat16),
                pltpu.VMEM((n_local, LANES), F32),
                pltpu.VMEM((cols, dim), jnp.bfloat16),
                pltpu.VMEM((group, crows + 8, LANES), F32),
                pltpu.VMEM((8, LANES), F32),
                pltpu.VMEM((group, 8, LANES), F32),
                pltpu.SemaphoreType.DMA((3,)),
                pltpu.SemaphoreType.DMA,
                pltpu.SemaphoreType.DMA,
                pltpu.SemaphoreType.DMA((group,)),
                pltpu.SemaphoreType.DMA((group,)),
                pltpu.SemaphoreType.DMA((group,)),
                pltpu.SemaphoreType.DMA((group,)),
                pltpu.SemaphoreType.DMA,
            ],
            compiler_params=pltpu.CompilerParams(
                collective_id=0, has_side_effects=True, vmem_limit_bytes=60 * 1024 * 1024
            ),
            name="knn_exchange",
        )(temperature, queries, tok_sorted.reshape(n_local // LANES, LANES), inv, key_shard, w_shard.T)

        fast, over = pl.pallas_call(
            functools.partial(_finish_kernel, cfg),
            out_shape=(jax.ShapeDtypeStruct((rows, cols), F32), jax.ShapeDtypeStruct((1,), jnp.int32)),
            in_specs=[smem, vmem, vmem, hbm],
            out_specs=(vmem, smem),
            scratch_shapes=[pltpu.VMEM((vrows, LANES), F32)] * 4
            + [
                pltpu.VMEM((group, crows, LANES), F32),
                pltpu.VMEM((cols, LANES), F32),
                pltpu.VMEM((group, 8, LANES), jnp.int32),
                pltpu.SMEM((group, 8, LANES), jnp.int32),
                pltpu.SemaphoreType.DMA,
                pltpu.SemaphoreType.DMA,
            ],
            compiler_params=pltpu.CompilerParams(vmem_limit_bytes=60 * 1024 * 1024),
            name="knn_finish",
        )(mix_weight, stats, recv, logits)

        args = (queries, w_shard, key_shard, tok_shard, temperature, mix_weight)
        return lax.cond(over[0] > 0, lambda: dense_path(*args), lambda: fast)

    return jax.shard_map(
        local_step,
        mesh=mesh,
        in_specs=(P("data", None), P(None, "model"), P("model", None), P("model"), P(), P()),
        out_specs=P("data", "model"),
        check_vma=False,
    )
```

```python
import functools

import jax
import jax.numpy as jnp
from jax import lax
from jax.experimental import pallas as pl
from jax.experimental.pallas import tpu as pltpu
from jax.sharding import PartitionSpec as P

MESH = pl.DeviceIdType.MESH
LANES = 128
BLK = 1024
SUB = 512
F32 = jnp.float32


DUP = 1 << 16
TILE_ROWS = 16


def _exchange_kernel(
    cfg, tau_ref, q_ref, sorted_ref, inv_hbm, keys_hbm, w_hbm,
    recv_ref, stats_out, logits_ref,
    q4_ref, tok_ref, inv_ref, isem, start_vmem, start_ref, stsem, kbuf, scores, wbuf, send, stats, stats_recv,
    ksem, wsem, lsem, send_sem, recv_sem, ssend_sem, srecv_sem, osem,
):
    group, rows, cap, cols, copies, vrows, side = cfg
    me = lax.axis_index("model")
    n_local = keys_hbm.shape[0]
    nblk = n_local // BLK
    crows = cap // copies
    tile = TILE_ROWS * copies
    qrows = q_ref.shape[0]

    barrier = pltpu.get_barrier_semaphore()

    @pl.loop(1, group)
    def _(k):
        peer = lax.rem(me + k, group)
        pl.semaphore_signal(barrier, inc=1, device_id={"model": peer}, device_id_type=MESH)

    def key_copy(b, slot):
        return pltpu.make_async_copy(keys_hbm.at[pl.ds(b * BLK, BLK), :], kbuf.at[slot], ksem.at[slot])

    key_copy(0, 0).start()
    key_copy(1, 1).start()
    w_copy = pltpu.make_async_copy(w_hbm, wbuf, wsem)
    inv_copy = pltpu.make_async_copy(inv_hbm, inv_ref.at[pl.ds(0, n_local)], isem)
    inv_copy.start()
    for i in range(tile):
        inv_ref[n_local + i] = 0
    tau = tau_ref[0]

    qt = jnp.concatenate([q_ref[...].astype(F32)] * copies, axis=0)
    for j in range(qt.shape[1] // LANES):
        q4_ref[j * LANES:(j + 1) * LANES, :] = qt[:, j * LANES:(j + 1) * LANES].T.astype(jnp.bfloat16)
    krows = sorted_ref.shape[0]
    tok_ref[:krows, :] = sorted_ref[...]
    tok_ref[krows:, :] = jnp.zeros((tok_ref.shape[0] - krows, LANES), jnp.int32)
    start_vmem[...] = jnp.zeros(start_vmem.shape, jnp.int32)
    for d in range(group + 1):
        below = jnp.where(sorted_ref[...] < d * cols, 1, 0).reshape(krows // 8, 8, LANES)
        part = below[0]
        for i in range(1, krows // 8):
            part = part + below[i]
        for i in (4, 2, 1):
            part = part[:i] + part[i:2 * i]
        start_vmem[d:d + 1, :] = part
    counts = start_vmem[...]
    turn = LANES // 2
    while turn:
        counts = counts + pltpu.roll(counts, turn, axis=1)
        turn //= 2
    start_vmem[...] = counts
    start_copy = pltpu.make_async_copy(start_vmem, start_ref, stsem)

    def block(b, best):
        slot = lax.rem(b, 3)

        @pl.when(b + 2 < nblk)
        def _():
            key_copy(b + 2, lax.rem(b + 2, 3)).start()

        @pl.when(b == 1)
        def _():
            start_copy.start()

        key_copy(b, slot).wait()

        def piece(p, best):
            x = kbuf[slot, pl.ds(p * SUB, SUB), :]
            dot = jnp.dot(x, q4_ref[...], preferred_element_type=F32)
            xf = x.astype(F32)
            sq = jnp.square(xf[:, :LANES])
            for j in range(1, x.shape[1] // LANES):
                sq = sq + jnp.square(xf[:, j * LANES:(j + 1) * LANES])
            norm = jnp.sum(sq, axis=1, keepdims=True)
            s = (2.0 * dot - norm) / tau
            scores[pl.ds(b * BLK + p * SUB, SUB), :] = s
            return jnp.maximum(best, jnp.max(s.reshape(SUB // 8, 8, LANES), axis=0))

        return lax.fori_loop(0, BLK // SUB, piece, best)

    best = lax.fori_loop(0, nblk, block, jnp.full((8, LANES), -jnp.inf, F32))
    w_copy.start()
    row_max = jnp.max(best, axis=0, keepdims=True)

    inv_copy.wait()
    start_copy.wait()
    pl.semaphore_wait(barrier, group - 1)

    lane_group = lax.broadcasted_iota(jnp.int32, (1, LANES), 1) // qrows
    entry = (
        lax.broadcasted_iota(jnp.int32, (crows, LANES), 0) * copies
        + lax.broadcasted_iota(jnp.int32, (crows, LANES), 1) // qrows
    )
    id_pos = lax.broadcasted_iota(jnp.int32, (8, LANES), 0) * LANES + lax.broadcasted_iota(jnp.int32, (8, LANES), 1)
    id_lane = lax.broadcasted_iota(jnp.int32, (8, LANES), 1)

    def block_send(k, dest):
        return pltpu.make_async_remote_copy(
            src_ref=send.at[k], dst_ref=recv_ref.at[me], send_sem=send_sem.at[k], recv_sem=recv_sem.at[me],
            device_id={"model": dest}, device_id_type=MESH,
        )

    def far_first(i, n):
        odd = lax.rem(i, 2)
        return n // 2 + (1 - odd) * lax.div(i, 2) - odd * lax.div(i + 1, 2)

    def dest_of(j):
        if side == 0:
            return lax.rem(me + 1 + j, group)
        y, x, c = lax.div(me, 2 * side), lax.rem(lax.div(me, 2), side), lax.rem(me, 2)
        dy = far_first(lax.rem(j, side), side)
        dx = far_first(lax.rem(lax.div(j, 2 * side) + lax.rem(j, side) + 1, side), side)
        dc = 1 - lax.rem(lax.div(j, side), 2)
        return (lax.rem(y + dy, side) * side + lax.rem(x + dx, side)) * 2 + lax.rem(c + dc, 2)

    def pack(k, dest, total):
        first = jnp.clip(start_ref[dest, 0], 0, n_local)
        count = start_ref[dest + 1, 0] - first

        @pl.loop(0, crows // TILE_ROWS)
        def _(t):
            base = jnp.minimum(first + t * tile, n_local)
            near = [inv_ref.at[pl.ds(i, n_local + 1)][base] for i in range(tile)]
            for r in range(TILE_ROWS):
                parts = [scores[pl.ds(near[r * copies + g], 1), :] for g in range(copies)]
                row = parts[copies - 1]
                for g in range(copies - 2, -1, -1):
                    row = jnp.where(lane_group == g, parts[g], row)
                send[k, pl.ds(t * TILE_ROWS + r, 1), :] = row

        w = jnp.where(entry < count, jnp.exp(send[k, :crows, :] - row_max), 0.0)
        send[k, :crows, :] = w
        shift = lax.rem(first, LANES)
        at = lax.div(first, LANES)
        low = pltpu.roll(tok_ref[pl.ds(at, 8), :], LANES - shift, axis=1)
        high = pltpu.roll(tok_ref[pl.ds(at + 1, 8), :], LANES - shift, axis=1)
        tok = jnp.where(id_lane < LANES - shift, low, high) - dest * cols
        tok = jnp.where(id_pos < count, tok, cols + lax.rem(lax.div(id_pos, copies), TILE_ROWS))
        send[k, crows:crows + 8, :] = jnp.where(id_pos < 7 * LANES, tok, count).astype(F32)
        return total + jnp.sum(w.reshape(crows // 8, 8, LANES), axis=0)

    def step(j, total):
        total = pack(j, dest_of(j), total)
        block_send(j - 1, dest_of(j - 1)).start()
        return total

    total = pack(0, dest_of(0), jnp.zeros((8, LANES), F32))
    total = lax.fori_loop(1, group - 1, step, total)
    total = pack(group - 1, me, total)
    block_send(group - 2, dest_of(group - 2)).start()
    own = pltpu.make_async_copy(send.at[group - 1], recv_ref.at[me], lsem)

    w_copy.wait()
    def head(at, size, carry):
        lm_max, lm_sum = carry
        x = jnp.dot(wbuf[pl.ds(at, size), :], q4_ref[...], preferred_element_type=F32)
        logits_ref[pl.ds(at, size), :] = x
        new = jnp.maximum(lm_max, jnp.max(x, axis=0, keepdims=True))
        return new, lm_sum * jnp.exp(lm_max - new) + jnp.sum(jnp.exp(x - new), axis=0, keepdims=True)

    carry = (jnp.full((1, LANES), -jnp.inf, F32), jnp.zeros((1, LANES), F32))
    carry = lax.fori_loop(0, cols // SUB, lambda i, c: head(i * SUB, SUB, c), carry)
    if cols % SUB:
        carry = head(cols // SUB * SUB, cols % SUB, carry)
    lm_max_row, lm_sum_row = carry

    def worst(d, c):
        return jnp.maximum(c, start_ref[d + 1, 0] - start_ref[d, 0])

    most = lax.fori_loop(0, group, worst, jnp.int32(0))
    over = jnp.where(most > cap, 1.0, 0.0).astype(F32)
    stats[0:1, :] = row_max
    stats[1:2, :] = jnp.sum(total, axis=0, keepdims=True)
    stats[2:3, :] = lm_max_row
    stats[3:4, :] = lm_sum_row
    stats[4:5, :] = jnp.full((1, LANES), over, F32)
    stats[5:8, :] = jnp.zeros((3, LANES), F32)
    own.start()
    own.wait()

    def stat_send(k, dest):
        return pltpu.make_async_remote_copy(
            src_ref=stats, dst_ref=stats_recv.at[me], send_sem=ssend_sem.at[k], recv_sem=srecv_sem.at[me],
            device_id={"model": dest}, device_id_type=MESH,
        )

    @pl.loop(1, group)
    def _(k):
        stat_send(k, lax.rem(me + k, group)).start()

    stats_recv[me] = stats[...]

    @pl.loop(1, group)
    def _(k):
        src = lax.rem(me + group - k, group)
        pltpu.make_async_remote_copy(
            src_ref=stats, dst_ref=stats_recv.at[src], send_sem=ssend_sem.at[k], recv_sem=srecv_sem.at[src],
            device_id={"model": src}, device_id_type=MESH,
        ).wait_recv()
        pltpu.make_async_remote_copy(
            src_ref=send.at[k - 1], dst_ref=recv_ref.at[src], send_sem=send_sem.at[k - 1], recv_sem=recv_sem.at[src],
            device_id={"model": src}, device_id_type=MESH,
        ).wait_recv()

    @pl.loop(1, group)
    def _(k):
        block_send(k - 1, dest_of(k - 1)).wait_send()
        stat_send(k, lax.rem(me + k, group)).wait_send()

    stats_out[...] = stats_recv[...]


def _finish_kernel(
    cfg, mix_ref, stats_ref, recv_ref, logits_hbm, out_ref, over_ref,
    hist0, hist1, hist2, hist3, scaled, logits_ref, idbuf, ids, sem, lsem,
):
    group, rows, cap, cols, copies, vrows, side = cfg
    crows = cap // copies
    hists = (hist0, hist1, hist2, hist3)
    logits_copy = pltpu.make_async_copy(logits_hbm, logits_ref, lsem)
    logits_copy.start()
    tile = TILE_ROWS * copies
    lane3 = lax.broadcasted_iota(jnp.int32, (8, LANES), 1)
    row3 = lax.broadcasted_iota(jnp.int32, (8, LANES), 0)
    for s in range(group):
        v = recv_ref[s, crows:crows + 8, :].astype(jnp.int32)
        same = (v == pltpu.roll(v, LANES - copies, axis=1)) & (lax.rem(lane3, tile) < tile - copies)
        flag = jnp.where(same, 1, 0)
        step = tile // 2
        while step:
            flag = flag | pltpu.roll(flag, LANES - step, axis=1)
            step //= 2
        count = jnp.sum(jnp.where((lane3 == 0) & (row3 == 7), v, 0).astype(F32)).astype(jnp.int32)
        flag = jnp.where(row3 * LANES + lane3 < count, flag, 2)
        idbuf[s] = v + jnp.where((lax.rem(lane3, tile) == 0) & (row3 < 7), flag * DUP, 0)
    id_copy = pltpu.make_async_copy(idbuf, ids, sem)

    st = stats_ref[...]
    m_all = st[:, 0, :]
    m = jnp.max(m_all, axis=0, keepdims=True)
    scale = jnp.exp(m_all - m)
    z = jnp.sum(st[:, 1, :] * scale, axis=0, keepdims=True)
    lm_all = st[:, 2, :]
    lm = jnp.max(lm_all, axis=0, keepdims=True)
    lmz = jnp.sum(st[:, 3, :] * jnp.exp(lm_all - lm), axis=0, keepdims=True)

    @pl.loop(0, vrows // 32)
    def _(i):
        for h in hists:
            h[pl.ds(i * 32, 32), :] = jnp.zeros((32, LANES), F32)

    id_copy.start()
    for s in range(group):
        scaled[s] = recv_ref[s, :crows, :] * scale[s:s + 1, :]
    id_copy.wait()

    per = LANES // tile

    def tile_add(s, near, t, k):
        code = near[k * tile]
        at = lambda i: near[k * tile + i] if i else code & (DUP - 1)

        @pl.when(code < DUP)
        def _():
            rows_ = [scaled[s, pl.ds(t * TILE_ROWS + r, 1), :] for r in range(TILE_ROWS)]
            for g in range(copies):
                at_g = [at(r * copies + g) for r in range(TILE_ROWS)]
                new = [hists[g][pl.ds(v, 1), :] + row for v, row in zip(at_g, rows_)]
                for v, x in zip(at_g, new):
                    hists[g][pl.ds(v, 1), :] = x

        @pl.when((code >= DUP) & (code < 2 * DUP))
        def _():
            for r in range(TILE_ROWS):
                row = scaled[s, pl.ds(t * TILE_ROWS + r, 1), :]
                for g in range(copies):
                    v = at(r * copies + g)
                    hists[g][pl.ds(v, 1), :] = hists[g][pl.ds(v, 1), :] + row

    @pl.loop(0, group)
    def _(s):
        @pl.loop(0, lax.div(jnp.minimum(ids[s, 7, 0], cap) + (LANES - 1), LANES))
        def _(sub):
            near = [ids.at[:, :, pl.ds(i, 1)][s, sub, 0] for i in range(LANES)]
            for k in range(per):
                tile_add(s, near, sub * per + k, k)

    over_ref[0] = jnp.max(st[:, 4, :]).astype(jnp.int32)
    logits_copy.wait()

    qrows = out_ref.shape[0]
    lane = lax.broadcasted_iota(jnp.int32, (LANES, LANES), 1)
    z8 = jnp.broadcast_to(z, (8, LANES))
    z_all = z8
    for g in range(1, copies):
        z_all = z_all + pltpu.roll(z8, g * qrows, axis=1)
    mix = mix_ref[0]
    a = mix / z_all[0:1]
    b = jnp.where(lane[0:1] < qrows, (1.0 - mix) / lmz, 0.0)
    for c in range(pl.cdiv(cols, LANES)):
        width = min(LANES, cols - c * LANES)
        part = slice(c * LANES, c * LANES + width)
        acc = hists[0][part, :]
        for g in range(1, copies):
            acc = jnp.where(lane[:width] >= g * qrows, hists[g][part, :], acc)
        x = acc * a + jnp.exp(logits_ref[part, :] - lm) * b
        if width < LANES:
            x = jnp.concatenate([x, jnp.zeros((LANES - width, LANES), F32)], axis=0)
        tr = x.T
        p = tr[:qrows]
        for g in range(1, copies):
            p = p + tr[g * qrows:(g + 1) * qrows]
        out_ref[:, part] = jnp.log(p[:, :width])


def solution(mesh):
    group = mesh.shape["model"]

    def dense_path(queries, w_shard, key_shard, tok_shard, temperature, mix_weight):
        row_count = queries.shape[0]
        cols = w_shard.shape[1]
        cross_dot = jnp.einsum("bd,nd->bn", queries, key_shard, preferred_element_type=F32)
        key_sq = jnp.sum(jnp.square(key_shard.astype(F32)), axis=1)
        scores = (2.0 * cross_dot - key_sq[None, :]) / temperature[0]
        row_max = lax.pmax(jnp.max(scores, axis=1), "model")
        weights = jnp.exp(scores - row_max[:, None])
        row_total = lax.psum(jnp.sum(weights, axis=1), "model")
        local_hist = jnp.zeros((row_count, cols * group), F32).at[:, tok_shard].add(weights)
        pieces = jnp.transpose(local_hist.reshape(row_count, group, cols), (1, 0, 2))
        histogram = jnp.sum(lax.all_to_all(pieces, "model", 0, 0), axis=0)
        logits = jnp.dot(queries, w_shard, preferred_element_type=F32)
        lm_max = lax.pmax(jnp.max(logits, axis=1), "model")
        lm_exp = jnp.exp(logits - lm_max[:, None])
        lm_total = lax.psum(jnp.sum(lm_exp, axis=1), "model")
        mix = mix_weight[0]
        return jnp.log(mix * (histogram / row_total[:, None]) + (1.0 - mix) * (lm_exp / lm_total[:, None]))

    def local_step(queries, w_shard, key_shard, tok_shard, temperature, mix_weight):
        rows, dim = queries.shape
        n_local = key_shard.shape[0]
        cols = w_shard.shape[1]
        copies = LANES // rows
        mean = n_local // group
        cap = -(-int(mean + 5.6 * mean ** 0.5) // (TILE_ROWS * copies)) * (TILE_ROWS * copies)
        crows = cap // copies
        vrows = -(-(cols + TILE_ROWS) // 32) * 32
        side = int((group // 2) ** 0.5)
        side = side if side * side * 2 == group and side in (2, 4) else 0
        cfg = (group, rows, cap, cols, copies, vrows, side)
        srows = -(-(group + 1) // 8) * 8
        assert n_local % (8 * LANES) == 0 and cap <= 7 * LANES and vrows < DUP
        tok_sorted, inv = lax.sort((tok_shard, lax.iota(jnp.int32, n_local)), num_keys=1)

        smem = pl.BlockSpec(memory_space=pltpu.SMEM)
        vmem = pl.BlockSpec(memory_space=pltpu.VMEM)
        hbm = pl.BlockSpec(memory_space=pl.ANY)
        recv, stats, logits = pl.pallas_call(
            functools.partial(_exchange_kernel, cfg),
            out_shape=(
                jax.ShapeDtypeStruct((group, crows + 8, LANES), F32),
                jax.ShapeDtypeStruct((group, 8, LANES), F32),
                jax.ShapeDtypeStruct((cols, LANES), F32),
            ),
            in_specs=[smem, vmem, vmem, hbm, hbm, hbm],
            out_specs=(hbm, vmem, vmem),
            scratch_shapes=[
                pltpu.VMEM((dim, LANES), jnp.bfloat16),
                pltpu.VMEM((n_local // LANES + 16, LANES), jnp.int32),
                pltpu.SMEM((n_local + TILE_ROWS * copies,), jnp.int32),
                pltpu.SemaphoreType.DMA,
                pltpu.VMEM((srows, LANES), jnp.int32),
                pltpu.SMEM((srows, LANES), jnp.int32),
                pltpu.SemaphoreType.DMA,
                pltpu.VMEM((3, BLK, dim), jnp.bfloat16),
                pltpu.VMEM((n_local, LANES), F32),
                pltpu.VMEM((cols, dim), jnp.bfloat16),
                pltpu.VMEM((group, crows + 8, LANES), F32),
                pltpu.VMEM((8, LANES), F32),
                pltpu.VMEM((group, 8, LANES), F32),
                pltpu.SemaphoreType.DMA((3,)),
                pltpu.SemaphoreType.DMA,
                pltpu.SemaphoreType.DMA,
                pltpu.SemaphoreType.DMA((group,)),
                pltpu.SemaphoreType.DMA((group,)),
                pltpu.SemaphoreType.DMA((group,)),
                pltpu.SemaphoreType.DMA((group,)),
                pltpu.SemaphoreType.DMA,
            ],
            compiler_params=pltpu.CompilerParams(
                collective_id=0, has_side_effects=True, vmem_limit_bytes=60 * 1024 * 1024
            ),
            name="knn_exchange",
        )(temperature, queries, tok_sorted.reshape(n_local // LANES, LANES), inv, key_shard, w_shard.T)

        fast, over = pl.pallas_call(
            functools.partial(_finish_kernel, cfg),
            out_shape=(jax.ShapeDtypeStruct((rows, cols), F32), jax.ShapeDtypeStruct((1,), jnp.int32)),
            in_specs=[smem, vmem, vmem, hbm],
            out_specs=(vmem, smem),
            scratch_shapes=[pltpu.VMEM((vrows, LANES), F32)] * 4
            + [
                pltpu.VMEM((group, crows, LANES), F32),
                pltpu.VMEM((cols, LANES), F32),
                pltpu.VMEM((group, 8, LANES), jnp.int32),
                pltpu.SMEM((group, 8, LANES), jnp.int32),
                pltpu.SemaphoreType.DMA,
                pltpu.SemaphoreType.DMA,
            ],
            compiler_params=pltpu.CompilerParams(vmem_limit_bytes=60 * 1024 * 1024),
            name="knn_finish",
        )(mix_weight, stats, recv, logits)

        args = (queries, w_shard, key_shard, tok_shard, temperature, mix_weight)
        return lax.cond(over[0] > 0, lambda: dense_path(*args), lambda: fast)

    return jax.shard_map(
        local_step,
        mesh=mesh,
        in_specs=(P("data", None), P(None, "model"), P("model", None), P("model"), P(), P()),
        out_specs=P("data", "model"),
        check_vma=False,
    )
```
